512 devices in a mesh: slab: 2 (over y), date: 16 (over z), tile: 8 (over x), sub: 2 (over core).
Axes of the slice: x: 8, y: 2, z: 16, core: 2. Of those that a mesh axis runs over, the one named last changes fastest.
The devices are a block of a 8x8x16 slice.
Arguments:
- slc: bfloat16 [2, 100, 128, 8192], P(None, None, 'date', ('slab', 'tile', 'sub')), parts along dimension 3, may hold values from -300 to 300, as said below
- usable: int32 [100, 128, 8192], P(None, 'date', ('slab', 'tile', 'sub')), parts along dimension 2, may hold values 0 or 1
Outputs:
- coherence: bfloat16 [2, 32, 16, 16, 128, 128], P(None, ('slab', 'tile', 'sub'), 'date'), parts along dimension 1
- linked: float32 [2, 128, 8192], P(None, 'date', ('slab', 'tile', 'sub')), parts along dimension 2
The draws below stay inside these ranges and needn't reach their ends.
There are 2 independent parts, one for each index of `slab`. The reference program is written for one: setup_inputs(seed, part) draws one part's arguments, and reference() takes and returns one part's arrays. A program takes and returns all parts, laid end to end along the dimension named above; each array names one. Nothing has to cross between parts.
Inputs may be any that keep to these rules, and one draw needn't show every extreme that they name: `slc`: complex samples of a partly coherent stack.
All inputs are finite; a program needn't handle non-finite values. No bound on the sum of `usable` on one device may be relied on, other than what follows from the above.
Results may differ from the reference program's by a relative error of at most 0.0016.
Values may be sent and summed in bfloat16 or wider, within the bound.
A program may use at most 64 MiB of HBM per device.

```python
import math
import jax
import jax.numpy as jnp
from jax import lax

DATES = 128
LOOKS = 100
ITERS = 4
WD = 16
WT = 256
NG = 16
NB = 16
WIN = 4096


def rotate(common, phase):
    cosine = jnp.cos(phase)[None]
    sine_part = jnp.sin(phase)[None]
    return jnp.stack([common[0] * cosine - common[1] * sine_part, common[0] * sine_part + common[1] * cosine])


def draw_slc(key, part):
    subkeys = jax.random.split(key, 9)
    grid_shape = (DATES, WIN)
    amplitude = jnp.exp(jax.random.uniform(subkeys[0], grid_shape, jnp.float32, 0.0, math.log(10.0)))
    speckle = jnp.clip(jax.random.normal(subkeys[8], (2, LOOKS, DATES, WIN), jnp.float32), -4.0, 4.0)
    first_phase = jax.random.uniform(subkeys[1], grid_shape, jnp.float32, -math.pi, math.pi)
    second_phase = jax.random.uniform(subkeys[2], grid_shape, jnp.float32, -math.pi, math.pi)
    first_weight = jax.random.uniform(subkeys[3], (WIN,), jnp.float32, 0.3, 0.9)
    second_weight = jax.random.uniform(subkeys[4], (WIN,), jnp.float32, 0.1, 0.4)
    first_common = jnp.clip(jax.random.normal(subkeys[5], (2, LOOKS, 1, WIN), jnp.float32), -4.0, 4.0)
    second_common = jnp.clip(jax.random.normal(subkeys[6], (2, LOOKS, 1, WIN), jnp.float32), -4.0, 4.0)
    noise_weight = jnp.sqrt(jnp.maximum(1.0 - first_weight * first_weight - second_weight * second_weight, 0.05))
    sample = first_weight * rotate(first_common, first_phase) + second_weight * rotate(second_common, second_phase) + noise_weight * speckle
    return (amplitude * sample).astype(jnp.bfloat16)


def set_ends(drawn, stream_key, low, high):
    dims = drawn.shape
    place = [jax.random.randint(jax.random.fold_in(stream_key, axis), (), 0, dims[axis]) for axis in range(len(dims))]
    drawn = drawn.at[tuple(place)].set(low)
    longest = dims.index(max(dims))
    place[longest] = (place[longest] + 1) % dims[longest]
    return drawn.at[tuple(place)].set(high)


def setup_inputs(seed: int = 0, part: int = 0) -> dict:
    seeds = jax.random.split(jax.random.key(seed), 3)
    own_keys = jax.random.split(jax.random.fold_in(seeds[2], part), 3)
    return {
        "slc": draw_slc(jax.random.fold_in(jax.random.fold_in(seeds[2], part), 71), part),
        "usable": set_ends((jax.random.randint(own_keys[1], (LOOKS, DATES, WIN), 0, 4) < 3).astype(jnp.int32), jax.random.fold_in(own_keys[1], 1), 0, 1),
    }


def link_vectors(coherence):
    matrix = coherence.astype(jnp.float32)
    vec_real = jnp.ones((DATES, matrix.shape[1]), jnp.float32)
    vec_imag = jnp.zeros((DATES, matrix.shape[1]), jnp.float32)
    for step in range(ITERS):
        rr = jnp.einsum('wab,bw->aw', matrix[0], vec_real, precision=lax.Precision.HIGHEST)
        ii = jnp.einsum('wab,bw->aw', matrix[1], vec_imag, precision=lax.Precision.HIGHEST)
        ri = jnp.einsum('wab,bw->aw', matrix[0], vec_imag, precision=lax.Precision.HIGHEST)
        ir = jnp.einsum('wab,bw->aw', matrix[1], vec_real, precision=lax.Precision.HIGHEST)
        new_real = rr - ii
        new_imag = ri + ir
        scale = lax.rsqrt(lax.optimization_barrier(jnp.mean(new_real * new_real + new_imag * new_imag, axis=0)) + 1e-05)
        vec_real = new_real * scale[None]
        vec_imag = new_imag * scale[None]
    return jnp.stack([vec_real, vec_imag])

def window_block(operands):
    block, root = operands
    real_sum = jnp.einsum('law,lbw->wab', block[0], block[0]) + jnp.einsum('law,lbw->wab', block[1], block[1])
    imag_sum = jnp.einsum('law,lbw->wab', block[1], block[0]) - jnp.einsum('law,lbw->wab', block[0], block[1])
    factor = root.T[:, :, None] * root.T[:, None, :] * (1.0 / LOOKS)
    coherence = jnp.stack([real_sum * factor, imag_sum * factor]).astype(jnp.bfloat16)
    return (coherence, link_vectors(coherence))

def reference(slc, usable):
    masked = slc * usable.astype(jnp.bfloat16)[None]
    samples = masked.astype(jnp.float32)
    intensity = lax.optimization_barrier(jnp.mean(samples[0] * samples[0] + samples[1] * samples[1], axis=0)) + 1e-05
    inverse_root = lax.rsqrt(intensity)
    blocks = jnp.moveaxis(samples.reshape(2, LOOKS, DATES, NG, WT), 3, 0)
    roots = jnp.moveaxis(inverse_root.reshape(DATES, NG, WT), 1, 0)
    coherence, linked = lax.map(window_block, (blocks, roots))
    coherence = jnp.moveaxis(coherence, 1, 0)
    linked = jnp.moveaxis(linked, 0, 2).reshape(2, DATES, WIN)
    return (coherence.reshape(2, NG, NB, WD, DATES, DATES), linked)
```

```python
import functools

import jax
import jax.numpy as jnp
from jax import lax
from jax.experimental import pallas as pl
from jax.experimental.pallas import tpu as pltpu
from jax.sharding import PartitionSpec as P

ITERS = 4
MESH = pl.DeviceIdType.MESH
F32, BF16 = jnp.float32, jnp.bfloat16
T1, T2 = 16, 8
TILES = T1 + T2 + 1


def lane_iota(shape):
    return lax.broadcasted_iota(jnp.int32, shape, len(shape) - 1)


def pack(slc_ref, usable_ref, plane, split1, split2, send, looks, dates, blocks):
    rows = looks * dates

    def mask_step(l, carry):
        use = usable_ref[l].astype(F32)
        for c in range(2):
            masked = slc_ref[c, l].astype(F32) * use
            at = pl.ds(pl.multiple_of(c * rows + l * dates, 8), dates)
            for half in range(2):
                plane[half, at, :] = masked[:, half * 128:half * 128 + 128]
        return carry

    lax.fori_loop(0, looks, mask_step, 0, unroll=4)

    bit = (lane_iota((8, 8, 128)) // 8) % 2 == 1
    for half in range(2):

        def date_step(a, carry):
            def group(c, look, count):
                return plane[half, pl.ds(c * rows + look * dates + a, count, stride=dates), :]

            first = jnp.concatenate([group(c, 0, 64) for c in range(2)], axis=0)
            split1[pl.ds(half * 1024 + a, 128, stride=8), :] = first.T
            parts = []
            for c in range(2):
                for u in range(4):
                    rest = group(c, 64 + 8 * u, 8)
                    parts += [rest, rest]
            second = jnp.concatenate(parts, axis=0).T.reshape(8, 2, 8, 128)
            pairs = jnp.where(bit, second[:, 0], second[:, 1]).reshape(64, 128)
            split2[pl.ds(half * 512 + a, 64, stride=8), :] = pairs
            return carry

        lax.fori_loop(0, dates, date_step, 0)

    groups = [(c, r) for c in range(2) for r in range(4)]
    for half in range(2):
        left = [plane[half, c * rows + (96 + r) * dates:c * rows + (97 + r) * dates, :] for c, r in groups]
        for b in range(8):
            tile = jnp.zeros((8, 128), F32)
            for g, part in enumerate(left):
                shift = (16 * (g - b)) % 128
                moved = pltpu.roll(part, shift, 1) if shift else part
                tile = jnp.where(lane_iota((8, 128)) // 16 == g, moved, tile)
            send[half * 8 + b, T1 + T2] = tile.astype(BF16)

    def out_step(b, carry):
        one = split1[pl.ds(pl.multiple_of(b * 128, 128), 128), :].reshape(T1, 8, 128)
        two = split2[pl.ds(pl.multiple_of(b * 64, 64), 64), :].reshape(T2, 8, 128)
        send[b, 0:T1] = one.astype(BF16)
        send[b, T1:T1 + T2] = two.astype(BF16)
        return carry

    lax.fori_loop(0, blocks, out_step, 0)


def gram(recv, coherence, i, looks):
    lane = lane_iota((128, 128))
    one = recv[i].astype(F32).reshape(128, 128)
    pair = recv[T1 + i % 8].astype(F32).reshape(128, 128)
    rest = recv[T1 + T2].astype(F32).reshape(128, 128)
    in_pair = ((lane // 8) % 2 == 1) == (i < 8)
    two = jnp.where(in_pair, pair, jnp.where(lane % 16 == i, rest, 0.0))
    sign = jnp.where(lane < 64, 1.0, -1.0)
    plain = jnp.concatenate([one, two], axis=1).astype(BF16)
    turned = jnp.concatenate([pltpu.roll(one, 64, 1) * sign, pltpu.roll(two, 64, 1) * sign], axis=1).astype(BF16)
    both = jnp.concatenate([plain, turned], axis=0)
    cross = lax.dot_general(both, plain, (((1,), (1,)), ((), ())), preferred_element_type=F32)
    real, imag = cross[:128], cross[128:]
    eye = lax.broadcasted_iota(jnp.int32, (128, 128), 0) == lane
    diagonal = jnp.where(eye, real, 0.0)
    column = lax.rsqrt(jnp.sum(diagonal, axis=1, keepdims=True) * (1.0 / looks) + 1e-05)
    row = lax.rsqrt(jnp.sum(diagonal, axis=0, keepdims=True) * (1.0 / looks) + 1e-05)
    factor = column * row * (1.0 / looks)
    coherence[0, 0, 0, i] = (real * factor).astype(BF16)
    coherence[1, 0, 0, i] = (imag * factor).astype(BF16)


def link(coherence, windows):
    vec_real = jnp.ones((windows, 128), F32)
    vec_imag = jnp.zeros((windows, 128), F32)
    row = lax.broadcasted_iota(jnp.int32, (4 * windows, 256), 0) % windows
    for step in range(ITERS):
        high_real, high_imag = vec_real.astype(BF16).astype(F32), vec_imag.astype(BF16).astype(F32)
        low_real, low_imag = vec_real - high_real, vec_imag - high_imag
        lhs = jnp.concatenate(
            [
                jnp.concatenate([high_real, high_imag], axis=1),
                jnp.concatenate([low_real, low_imag], axis=1),
                jnp.concatenate([high_imag, -high_real], axis=1),
                jnp.concatenate([low_imag, -low_real], axis=1),
            ],
            axis=0,
        )
        total = jnp.zeros((4 * windows, 128), F32)
        for w in range(windows):
            stacked = jnp.concatenate([coherence[0, 0, 0, w], coherence[1, 0, 0, w]], axis=0)
            total += jnp.dot(jnp.where(row == w, lhs, 0.0).astype(BF16), stacked, preferred_element_type=F32)
        new_real = total[:windows] + total[windows:2 * windows]
        new_imag = total[2 * windows:3 * windows] + total[3 * windows:]
        power = jnp.sum(new_real * new_real + new_imag * new_imag, axis=1, keepdims=True) * (1.0 / 128)
        scale = lax.rsqrt(power + 1e-05)
        vec_real, vec_imag = new_real * scale, new_imag * scale
    return vec_real, vec_imag


def kernel(
    n, slc_ref, usable_ref, coherence, linked, plane, split1, split2, send, recv, turn, note, notes,
    send_sem, recv_sem, note_send, note_recv,
):
    looks, dates = slc_ref.shape[1], slc_ref.shape[2]
    me = lax.axis_index("date")
    barrier = pltpu.get_barrier_semaphore()
    order = []
    for k in range(n // 2, 0, -1):
        order += [k] if 2 * k == n else [k, n - k]
    for k in order:
        pl.semaphore_signal(barrier, inc=1, device_id={"date": lax.rem(me + k, n)}, device_id_type=MESH)

    pack(slc_ref, usable_ref, plane, split1, split2, send, looks, dates, n)
    pl.semaphore_wait(barrier, n - 1)

    def sample_copy(k):
        to = lax.rem(me + k, n)
        return pltpu.make_async_remote_copy(
            src_ref=send.at[to], dst_ref=recv.at[:, me], send_sem=send_sem.at[k], recv_sem=recv_sem.at[k],
            device_id={"date": to}, device_id_type=MESH,
        )

    for k in order:
        sample_copy(k).start()
    recv[:, me] = send[me]
    for k in order:
        source = lax.rem(me + n - k, n)
        pltpu.make_async_remote_copy(
            src_ref=send.at[source], dst_ref=recv.at[:, source], send_sem=send_sem.at[k], recv_sem=recv_sem.at[k],
            device_id={"date": source}, device_id_type=MESH,
        ).wait_recv()

    for i in range(T1):
        gram(recv, coherence, i, looks)
    vec_real, vec_imag = link(coherence, T1)

    rows = jnp.concatenate([vec_real] + [vec_imag] * 4 + [vec_real] * 3, axis=0)
    turn[...] = rows.T
    lane = lane_iota((2 * n, 128))
    message = jnp.zeros((2 * n, 128), F32)
    for q in range(4):
        message = jnp.where((8 - lane // 16) % 4 == q, turn[pl.ds(q, 2 * n, stride=4), :], message)
    for d in range(n):
        note[d] = message[2 * d:2 * d + 2]

    def note_copy(k):
        to = lax.rem(me + k, n)
        return pltpu.make_async_remote_copy(
            src_ref=note.at[to], dst_ref=notes.at[me], send_sem=note_send.at[k], recv_sem=note_recv.at[k],
            device_id={"date": to}, device_id_type=MESH,
        )

    for k in order:
        note_copy(k).start()
    notes[me] = note[me]
    for k in order:
        source = lax.rem(me + n - k, n)
        pltpu.make_async_remote_copy(
            src_ref=note.at[source], dst_ref=notes.at[source], send_sem=note_send.at[k], recv_sem=note_recv.at[k],
            device_id={"date": source}, device_id_type=MESH,
        ).wait_recv()

    lane = lane_iota((8, 128))
    for h in range(2):
        for half in range(2):
            tile = jnp.zeros((8, 128), F32)
            came = jnp.concatenate([notes[half * 8 + s, h:h + 1, :] for s in range(8)], axis=0)
            came = pltpu.roll(came, 0, 1, stride=16, stride_axis=0)
            for s in range(8):
                source = jnp.broadcast_to(came[s:s + 1], (8, 128))
                moved = pltpu.roll(source, 0, 1, stride=16, stride_axis=0)
                tile = jnp.where(lane // 16 == s, moved, tile)
            for c in range(2):
                linked[c, 4 * h:4 * h + 4, half * 128:half * 128 + 128] = tile[4 * c:4 * c + 4]
    for k in order:
        sample_copy(k).wait_send()
        note_copy(k).wait_send()


def solution(mesh):
    n = mesh.shape["date"]

    def step(slc, usable):
        dates, windows = slc.shape[2], slc.shape[3]
        rows = 2 * slc.shape[1] * dates
        per_device = windows // n
        vmem = pl.BlockSpec(memory_space=pltpu.VMEM)
        return pl.pallas_call(
            functools.partial(kernel, n),
            out_shape=(
                jax.ShapeDtypeStruct((2, 1, 1, per_device, n * dates, n * dates), BF16),
                jax.ShapeDtypeStruct((2, dates, windows), F32),
            ),
            in_specs=[vmem, vmem],
            out_specs=(vmem, vmem),
            scratch_shapes=[
                pltpu.VMEM((windows // 128, rows, 128), F32),
                pltpu.VMEM((windows * dates, 128), F32),
                pltpu.VMEM((windows * dates // 2, 128), F32),
                pltpu.VMEM((n, TILES, dates, 128), BF16),
                pltpu.VMEM((TILES, n, dates, 128), BF16),
                pltpu.VMEM((128, 128), F32),
                pltpu.VMEM((n, 2, 128), F32),
                pltpu.VMEM((n, 2, 128), F32),
                pltpu.SemaphoreType.DMA((n,)),
                pltpu.SemaphoreType.DMA((n,)),
                pltpu.SemaphoreType.DMA((n,)),
                pltpu.SemaphoreType.DMA((n,)),
            ],
            compiler_params=pltpu.CompilerParams(collective_id=0, has_side_effects=True),
        )(slc, usable)

    return jax.shard_map(
        step,
        mesh=mesh,
        in_specs=(
            P(None, None, "date", ("slab", "tile", "sub")),
            P(None, "date", ("slab", "tile", "sub")),
        ),
        out_specs=(
            P(None, ("slab", "tile", "sub"), "date", None, None, None),
            P(None, "date", ("slab", "tile", "sub")),
        ),
        check_vma=False,
    )
```

```python
import functools

import jax
import jax.numpy as jnp
from jax import lax
from jax.experimental import pallas as pl
from jax.experimental.pallas import tpu as pltpu
from jax.sharding import PartitionSpec as P

ITERS = 4
MESH = pl.DeviceIdType.MESH
F32, BF16 = jnp.float32, jnp.bfloat16
WINDOWS = 16
LOADS = 5
CHUNKS = ((0, 13), (13, 12))
TILES = 25
REST = 12


def places(i):
    chunk, spot = divmod(i % 8, 4)
    return CHUNKS[chunk][0] + 4 * (i // 8) + spot, CHUNKS[chunk][0] + 8 + spot


def lane_iota(shape):
    return lax.broadcasted_iota(jnp.int32, shape, len(shape) - 1)


def pack(slc_ref, usable_ref, plane, split1, split2, send, loads, looks, dates, blocks):
    rows = looks * dates
    step = looks // LOADS

    def mask_step(l, carry):
        use = usable_ref[l].astype(F32)
        for c in range(2):
            masked = slc_ref[c, l].astype(F32) * use
            at = pl.ds(pl.multiple_of(c * rows + l * dates, 8), dates)
            for half in range(2):
                plane[half, at, :] = masked[:, half * 128:half * 128 + 128]
        return carry

    with jax.named_scope("mask"):
        for piece, copies in enumerate(loads):
            for copy in copies:
                copy.wait()
            lax.fori_loop(piece * step, piece * step + step, mask_step, 0, unroll=4)

    bit = (lane_iota((8, 8, 128)) // 8) % 2 == 1
    groups = [(c, r) for c in range(2) for r in range(4)]
    for half in range(2):

        def group(a, c, look, count):
            return plane[half, pl.ds(c * rows + look * dates + a, count, stride=dates), :]

        def date_step(a, carry):
            first = jnp.concatenate([group(a, c, 0, 64) for c in range(2)], axis=0)
            split1[pl.ds(half * 1024 + a, 128, stride=8), :] = first.T
            parts = []
            for c in range(2):
                for u in range(4):
                    rest = group(a, c, 64 + 8 * u, 8)
                    parts += [rest, rest]
            second = jnp.concatenate(parts, axis=0).T.reshape(8, 2, 8, 128)
            pairs = jnp.where(bit, second[:, 0], second[:, 1]).reshape(64, 128)
            split2[pl.ds(half * 512 + a, 64, stride=8), :] = pairs
            return carry

        lax.fori_loop(0, dates, date_step, 0, unroll=4)

        left = [plane[half, c * rows + (96 + r) * dates:c * rows + (97 + r) * dates, :] for c, r in groups]
        for b in range(8):
            tile = jnp.zeros((8, 128), F32)
            for g, part in enumerate(left):
                shift = (16 * (g - b)) % 128
                moved = pltpu.roll(part, shift, 1) if shift else part
                tile = jnp.where(lane_iota((8, 128)) // 16 == g, moved, tile)
            send[half * 8 + b, REST] = tile.astype(BF16)

    def out_step(b, carry):
        one = split1[pl.ds(pl.multiple_of(b * 128, 128), 128), :].reshape(16, 8, 128).astype(BF16)
        two = split2[pl.ds(pl.multiple_of(b * 64, 64), 64), :].reshape(8, 8, 128).astype(BF16)
        for chunk, (base, _) in enumerate(CHUNKS):
            send[b, base:base + 4] = one[4 * chunk:4 * chunk + 4]
            send[b, base + 4:base + 8] = one[8 + 4 * chunk:12 + 4 * chunk]
            send[b, base + 8:base + 12] = two[4 * chunk:4 * chunk + 4]
        return carry

    with jax.named_scope("cast"):
        lax.fori_loop(0, blocks, out_step, 0)


def gram(recv, coherence, i, looks):
    lane = lane_iota((128, 128))
    own, shared = places(i)
    one = recv[own].astype(F32).reshape(128, 128)
    pair = recv[shared].astype(F32).reshape(128, 128)
    rest = recv[REST].astype(F32).reshape(128, 128)
    in_pair = ((lane // 8) % 2 == 1) == (i < 8)
    two = jnp.where(in_pair, pair, jnp.where(lane % 16 == i, rest, 0.0))
    sign = jnp.where(lane < 64, 1.0, -1.0)
    plain = jnp.concatenate([one, two], axis=1).astype(BF16)
    turned = jnp.concatenate([pltpu.roll(one, 64, 1) * sign, pltpu.roll(two, 64, 1) * sign], axis=1).astype(BF16)
    both = jnp.concatenate([plain, turned], axis=0)
    cross = lax.dot_general(both, plain, (((1,), (1,)), ((), ())), preferred_element_type=F32)
    real, imag = cross[:128], cross[128:]
    eye = lax.broadcasted_iota(jnp.int32, (128, 128), 0) == lane
    diagonal = jnp.where(eye, real, 0.0)
    column = lax.rsqrt(jnp.sum(diagonal, axis=1, keepdims=True) * (1.0 / looks) + 1e-05)
    row = lax.rsqrt(jnp.sum(diagonal, axis=0, keepdims=True) * (1.0 / looks) + 1e-05)
    factor = column * row * (1.0 / looks)
    coherence[0, 0, 0, i] = (real * factor).astype(BF16)
    coherence[1, 0, 0, i] = (imag * factor).astype(BF16)


def link(coherence, windows):
    row = lax.broadcasted_iota(jnp.int32, (4 * windows, 256), 0) % windows
    real, imag = jnp.ones((windows, 128), F32), jnp.zeros((windows, 128), F32)
    scale = None
    for step in range(ITERS):
        high_real, high_imag = real.astype(BF16).astype(F32), imag.astype(BF16).astype(F32)
        low_real, low_imag = real - high_real, imag - high_imag
        lhs = jnp.concatenate(
            [
                jnp.concatenate([high_real, high_imag], axis=1),
                jnp.concatenate([low_real, low_imag], axis=1),
                jnp.concatenate([high_imag, -high_real], axis=1),
                jnp.concatenate([low_imag, -low_real], axis=1),
            ],
            axis=0,
        )
        total = jnp.zeros((4 * windows, 128), F32)
        for w in range(windows):
            stacked = jnp.concatenate([coherence[0, 0, 0, w], coherence[1, 0, 0, w]], axis=0)
            total += jnp.dot(jnp.where(row == w, lhs, 0.0).astype(BF16), stacked, preferred_element_type=F32)
        real = total[:windows] + total[windows:2 * windows]
        imag = total[2 * windows:3 * windows] + total[3 * windows:]
        if scale is not None:
            real, imag = real * scale, imag * scale
        scale = lax.rsqrt(jnp.sum(real * real + imag * imag, axis=1, keepdims=True) * (1.0 / 128) + 1e-05)
    return real * scale, imag * scale


def kernel(
    n, slc_hbm, usable_hbm, coherence, notes, slc_ref, usable_ref, plane, split1, split2, send, recv, turn, note,
    load_sem, send_sem, recv_sem, note_send, note_recv,
):
    looks, dates = slc_ref.shape[1], slc_ref.shape[2]
    me = lax.axis_index("date")
    barrier = pltpu.get_barrier_semaphore()
    order = []
    for k in range(n // 2, 0, -1):
        order += [k] if 2 * k == n else [k, n - k]
    loads = []
    for piece in range(LOADS):
        part = pl.ds(piece * (looks // LOADS), looks // LOADS)
        loads.append([
            pltpu.make_async_copy(slc_hbm.at[0, part], slc_ref.at[0, part], load_sem.at[piece, 0]),
            pltpu.make_async_copy(slc_hbm.at[1, part], slc_ref.at[1, part], load_sem.at[piece, 1]),
            pltpu.make_async_copy(usable_hbm.at[part], usable_ref.at[part], load_sem.at[piece, 2]),
        ])
        for copy in loads[-1]:
            copy.start()
    for k in order:
        pl.semaphore_signal(barrier, inc=1, device_id={"date": lax.rem(me + k, n)}, device_id_type=MESH)

    pack(slc_ref, usable_ref, plane, split1, split2, send, loads, looks, dates, n)
    with jax.named_scope("barrier"):
        pl.semaphore_wait(barrier, n - 1)

    def sample_copy(k, chunk, to, slot):
        tiles = pl.ds(*CHUNKS[chunk])
        return pltpu.make_async_remote_copy(
            src_ref=send.at[to, tiles], dst_ref=recv.at[tiles, slot], send_sem=send_sem.at[0], recv_sem=recv_sem.at[chunk, k],
            device_id={"date": to}, device_id_type=MESH,
        )

    with jax.named_scope("start"):
        for chunk in range(2):
            for k in order:
                sample_copy(k, chunk, lax.rem(me + k, n), me).start()
        recv[:, me] = send[me]
    for chunk in range(2):
        with jax.named_scope("receive"):
            for k in order:
                source = lax.rem(me + n - k, n)
                sample_copy(k, chunk, source, source).wait_recv()
        with jax.named_scope("gram"):
            for i in range(WINDOWS):
                if (i % 8) // 4 == chunk:
                    gram(recv, coherence, i, looks)
    with jax.named_scope("link"):
        vec_real, vec_imag = link(coherence, WINDOWS)

    with jax.named_scope("note"):
        rows = jnp.concatenate([vec_real] + [vec_imag] * 4 + [vec_real] * 3, axis=0)
        turn[...] = rows.T
        lane = lane_iota((2 * n, 128))
        message = jnp.zeros((2 * n, 128), F32)
        for q in range(4):
            message = jnp.where((8 - lane // 16) % 4 == q, turn[pl.ds(q, 2 * n, stride=4), :], message)
        for d in range(n):
            note[d] = message[2 * d:2 * d + 2]

    def note_copy(k):
        to = lax.rem(me + k, n)
        return pltpu.make_async_remote_copy(
            src_ref=note.at[to], dst_ref=notes.at[me], send_sem=note_send.at[0], recv_sem=note_recv.at[k],
            device_id={"date": to}, device_id_type=MESH,
        )

    with jax.named_scope("notes"):
        for k in order:
            note_copy(k).start()
        notes[me] = note[me]
        pltpu.make_async_copy(send.at[0:n - 1], send.at[0:n - 1], send_sem.at[0]).wait()
        for k in order:
            source = lax.rem(me + n - k, n)
            pltpu.make_async_remote_copy(
                src_ref=note.at[source], dst_ref=notes.at[source], send_sem=note_send.at[0], recv_sem=note_recv.at[k],
                device_id={"date": source}, device_id_type=MESH,
            ).wait_recv()

    pltpu.make_async_copy(note.at[0:n - 1], note.at[0:n - 1], note_send.at[0]).wait()


def store(coherence, notes, coherence_out, linked_out, linked, sem):
    copies = [pltpu.make_async_copy(coherence.at[:, :, :, i], coherence_out.at[:, :, :, i], sem.at[i]) for i in range(WINDOWS)]
    for copy in copies:
        copy.start()
    lane = lane_iota((8, 128))
    for h in range(2):
        for half in range(2):
            tile = jnp.zeros((8, 128), F32)
            came = jnp.concatenate([notes[half * 8 + s, h:h + 1, :] for s in range(8)], axis=0)
            came = pltpu.roll(came, 0, 1, stride=16, stride_axis=0)
            for s in range(8):
                source = jnp.broadcast_to(came[s:s + 1], (8, 128))
                moved = pltpu.roll(source, 0, 1, stride=16, stride_axis=0)
                tile = jnp.where(lane // 16 == s, moved, tile)
            for c in range(2):
                linked[c, 4 * h:4 * h + 4, half * 128:half * 128 + 128] = tile[4 * c:4 * c + 4]
    copies.append(pltpu.make_async_copy(linked, linked_out, sem.at[WINDOWS]))
    copies[-1].start()
    for copy in copies:
        copy.wait()


def solution(mesh):
    n = mesh.shape["date"]

    def step(slc, usable):
        dates, windows = slc.shape[2], slc.shape[3]
        rows = 2 * slc.shape[1] * dates
        per_device = windows // n
        vmem, hbm = pl.BlockSpec(memory_space=pltpu.VMEM), pl.BlockSpec(memory_space=pl.ANY)
        coherence_shape, linked_shape = (2, 1, 1, per_device, n * dates, n * dates), (2, dates, windows)
        coherence, notes = pl.pallas_call(
            functools.partial(kernel, n),
            out_shape=(pltpu.VMEM(coherence_shape, BF16), pltpu.VMEM((n, 2, 128), F32)),
            in_specs=[hbm, hbm],
            out_specs=(vmem, vmem),
            scratch_shapes=[
                pltpu.VMEM(slc.shape, BF16),
                pltpu.VMEM(usable.shape, jnp.int32),
                pltpu.VMEM((windows // 128, rows, 128), F32),
                pltpu.VMEM((windows * dates, 128), F32),
                pltpu.VMEM((windows * dates // 2, 128), F32),
                pltpu.VMEM((n, TILES, dates, 128), BF16),
                pltpu.VMEM((TILES, n, dates, 128), BF16),
                pltpu.VMEM((128, 128), F32),
                pltpu.VMEM((n, 2, 128), F32),
                pltpu.SemaphoreType.DMA((LOADS, 3)),
                pltpu.SemaphoreType.DMA((1,)),
                pltpu.SemaphoreType.DMA((2, n)),
                pltpu.SemaphoreType.DMA((1,)),
                pltpu.SemaphoreType.DMA((n,)),
            ],
            compiler_params=pltpu.CompilerParams(collective_id=0, has_side_effects=True),
        )(slc, usable)
        return pl.pallas_call(
            store,
            out_shape=(jax.ShapeDtypeStruct(coherence_shape, BF16), jax.ShapeDtypeStruct(linked_shape, F32)),
            in_specs=[vmem, vmem],
            out_specs=(hbm, hbm),
            scratch_shapes=[pltpu.VMEM(linked_shape, F32), pltpu.SemaphoreType.DMA((WINDOWS + 1,))],
        )(pltpu.with_memory_space_constraint(coherence, pltpu.VMEM), pltpu.with_memory_space_constraint(notes, pltpu.VMEM))

    return jax.shard_map(
        step,
        mesh=mesh,
        in_specs=(
            P(None, None, "date", ("slab", "tile", "sub")),
            P(None, "date", ("slab", "tile", "sub")),
        ),
        out_specs=(
            P(None, ("slab", "tile", "sub"), "date", None, None, None),
            P(None, "date", ("slab", "tile", "sub")),
        ),
        check_vma=False,
    )
```

```python
import functools

import jax
import jax.numpy as jnp
from jax import lax
from jax.experimental import pallas as pl
from jax.experimental.pallas import tpu as pltpu
from jax.sharding import PartitionSpec as P

ITERS = 4
MESH = pl.DeviceIdType.MESH
F32, BF16 = jnp.float32, jnp.bfloat16
WINDOWS = 16
LOADS = 5
CHUNKS = ((0, 13), (13, 12))
TILES = 25
REST = 12


def places(i):
    chunk, spot = divmod(i % 8, 4)
    return CHUNKS[chunk][0] + 4 * (i // 8) + spot, CHUNKS[chunk][0] + 8 + spot


def lane_iota(shape):
    return lax.broadcasted_iota(jnp.int32, shape, len(shape) - 1)


def pack(slc_ref, usable_ref, plane, split1, split2, send, loads, between, looks, dates, blocks):
    rows = looks * dates
    step = looks // LOADS

    def mask_step(l, carry):
        use = usable_ref[l].astype(F32)
        for c in range(2):
            masked = slc_ref[c, l].astype(F32) * use
            at = pl.ds(pl.multiple_of(c * rows + l * dates, 8), dates)
            for half in range(2):
                plane[half, at, :] = masked[:, half * 128:half * 128 + 128]
        return carry

    with jax.named_scope("mask"):
        for piece, copies in enumerate(loads):
            for copy in copies:
                copy.wait()
            lax.fori_loop(piece * step, piece * step + step, mask_step, 0, unroll=4)
    with jax.named_scope("greet"):
        between()

    bit = (lane_iota((8, 8, 128)) // 8) % 2 == 1
    groups = [(c, r) for c in range(2) for r in range(4)]
    for half in range(2):

        def group(a, c, look, count):
            return plane[half, pl.ds(c * rows + look * dates + a, count, stride=dates), :]

        def date_step(a, carry):
            first = jnp.concatenate([group(a, c, 0, 64) for c in range(2)], axis=0)
            split1[pl.ds(half * 1024 + a, 128, stride=8), :] = first.T
            parts = []
            for c in range(2):
                for u in range(4):
                    rest = group(a, c, 64 + 8 * u, 8)
                    parts += [rest, rest]
            second = jnp.concatenate(parts, axis=0).T.reshape(8, 2, 8, 128)
            pairs = jnp.where(bit, second[:, 0], second[:, 1]).reshape(64, 128)
            split2[pl.ds(half * 512 + a, 64, stride=8), :] = pairs
            return carry

        lax.fori_loop(0, dates, date_step, 0, unroll=4)

        left = [plane[half, c * rows + (96 + r) * dates:c * rows + (97 + r) * dates, :] for c, r in groups]
        for b in range(8):
            tile = jnp.zeros((8, 128), F32)
            for g, part in enumerate(left):
                shift = (16 * (g - b)) % 128
                moved = pltpu.roll(part, shift, 1) if shift else part
                tile = jnp.where(lane_iota((8, 128)) // 16 == g, moved, tile)
            send[half * 8 + b, REST] = tile.astype(BF16)

    def out_step(b, carry):
        one = split1[pl.ds(pl.multiple_of(b * 128, 128), 128), :].reshape(16, 8, 128).astype(BF16)
        two = split2[pl.ds(pl.multiple_of(b * 64, 64), 64), :].reshape(8, 8, 128).astype(BF16)
        for chunk, (base, _) in enumerate(CHUNKS):
            send[b, base:base + 4] = one[4 * chunk:4 * chunk + 4]
            send[b, base + 4:base + 8] = one[8 + 4 * chunk:12 + 4 * chunk]
            send[b, base + 8:base + 12] = two[4 * chunk:4 * chunk + 4]
        return carry

    with jax.named_scope("cast"):
        lax.fori_loop(0, blocks, out_step, 0)


def gram(recv, coherence, i, looks):
    lane = lane_iota((128, 128))
    own, shared = places(i)
    one = recv[own].astype(F32).reshape(128, 128)
    pair = recv[shared].astype(F32).reshape(128, 128)
    rest = recv[REST].astype(F32).reshape(128, 128)
    in_pair = ((lane // 8) % 2 == 1) == (i < 8)
    two = jnp.where(in_pair, pair, jnp.where(lane % 16 == i, rest, 0.0))
    sign = jnp.where(lane < 64, 1.0, -1.0)
    plain = jnp.concatenate([one, two], axis=1).astype(BF16)
    turned = jnp.concatenate([pltpu.roll(one, 64, 1) * sign, pltpu.roll(two, 64, 1) * sign], axis=1).astype(BF16)
    both = jnp.concatenate([plain, turned], axis=0)
    cross = lax.dot_general(both, plain, (((1,), (1,)), ((), ())), preferred_element_type=F32)
    real, imag = cross[:128], cross[128:]
    eye = lax.broadcasted_iota(jnp.int32, (128, 128), 0) == lane
    diagonal = jnp.where(eye, real, 0.0)
    column = lax.rsqrt(jnp.sum(diagonal, axis=1, keepdims=True) * (1.0 / looks) + 1e-05)
    row = lax.rsqrt(jnp.sum(diagonal, axis=0, keepdims=True) * (1.0 / looks) + 1e-05)
    factor = column * row * (1.0 / looks)
    coherence[0, 0, 0, i] = (real * factor).astype(BF16)
    coherence[1, 0, 0, i] = (imag * factor).astype(BF16)


def link(coherence, windows):
    row = lax.broadcasted_iota(jnp.int32, (4 * windows, 256), 0) % windows
    real, imag = jnp.ones((windows, 128), F32), jnp.zeros((windows, 128), F32)
    scale = None
    for step in range(ITERS):
        high_real, high_imag = real.astype(BF16).astype(F32), imag.astype(BF16).astype(F32)
        low_real, low_imag = real - high_real, imag - high_imag
        lhs = jnp.concatenate(
            [
                jnp.concatenate([high_real, high_imag], axis=1),
                jnp.concatenate([low_real, low_imag], axis=1),
                jnp.concatenate([high_imag, -high_real], axis=1),
                jnp.concatenate([low_imag, -low_real], axis=1),
            ],
            axis=0,
        )
        total = jnp.zeros((4 * windows, 128), F32)
        for w in range(windows):
            stacked = jnp.concatenate([coherence[0, 0, 0, w], coherence[1, 0, 0, w]], axis=0)
            total += jnp.dot(jnp.where(row == w, lhs, 0.0).astype(BF16), stacked, preferred_element_type=F32)
        real = total[:windows] + total[windows:2 * windows]
        imag = total[2 * windows:3 * windows] + total[3 * windows:]
        if scale is not None:
            real, imag = real * scale, imag * scale
        scale = lax.rsqrt(jnp.sum(real * real + imag * imag, axis=1, keepdims=True) * (1.0 / 128) + 1e-05)
    return real * scale, imag * scale


def kernel(
    n, slc_hbm, usable_hbm, coherence, notes, slc_ref, usable_ref, plane, split1, split2, send, recv, turn, note,
    load_sem, send_sem, recv_sem, note_send, note_recv, lower_sem, known_sem,
):
    looks, dates = slc_ref.shape[1], slc_ref.shape[2]
    me = lax.axis_index("date")
    barrier = pltpu.get_barrier_semaphore()
    order = []
    for k in range(n // 2, 0, -1):
        order += [k] if 2 * k == n else [k, n - k]
    loads = []
    for piece in range(LOADS):
        part = pl.ds(piece * (looks // LOADS), looks // LOADS)
        loads.append([
            pltpu.make_async_copy(slc_hbm.at[0, part], slc_ref.at[0, part], load_sem.at[piece, 0]),
            pltpu.make_async_copy(slc_hbm.at[1, part], slc_ref.at[1, part], load_sem.at[piece, 1]),
            pltpu.make_async_copy(usable_hbm.at[part], usable_ref.at[part], load_sem.at[piece, 2]),
        ])
        for copy in loads[-1]:
            copy.start()
    rank = lax.rem(me + n - 1, n)
    after, before = lax.rem(me + 1, n), lax.rem(me + n - 1, n)
    pl.semaphore_signal(barrier, inc=1, device_id={"date": before}, device_id_type=MESH)

    def greet():
        pl.semaphore_wait(barrier, 1)

        @pl.when(rank > 0)
        def _():
            pl.semaphore_wait(lower_sem, 1)

        for k in range(2, n):

            @pl.when(rank >= k)
            def _():
                pl.semaphore_signal(known_sem.at[k], inc=1, device_id={"date": lax.rem(me + n - k, n)}, device_id_type=MESH)

        @pl.when(rank < n - 1)
        def _():
            pl.semaphore_signal(lower_sem, inc=1, device_id={"date": after}, device_id_type=MESH)

    pack(slc_ref, usable_ref, plane, split1, split2, send, loads, lambda: pl.when(rank < n - 1)(greet), looks, dates, n)
    pl.when(rank == n - 1)(greet)

    def sample_copy(k, chunk, to, slot):
        tiles = pl.ds(*CHUNKS[chunk])
        return pltpu.make_async_remote_copy(
            src_ref=send.at[to, tiles], dst_ref=recv.at[tiles, slot], send_sem=send_sem.at[0], recv_sem=recv_sem.at[chunk, k],
            device_id={"date": to}, device_id_type=MESH,
        )

    with jax.named_scope("start"):
        for k in order:

            @pl.when(rank + k >= n)
            def _():
                for chunk in range(2):
                    sample_copy(k, chunk, lax.rem(me + k, n), me).start()

        recv[:, me] = send[me]
        for k in range(1, n):

            @pl.when(rank + k < n)
            def _():
                if k > 1:
                    pl.semaphore_wait(known_sem.at[k], 1)
                for chunk in range(2):
                    sample_copy(k, chunk, lax.rem(me + k, n), me).start()

    for chunk in range(2):
        with jax.named_scope("receive"):
            for k in order:
                source = lax.rem(me + n - k, n)
                sample_copy(k, chunk, source, source).wait_recv()
        with jax.named_scope("gram"):
            for i in range(WINDOWS):
                if (i % 8) // 4 == chunk:
                    gram(recv, coherence, i, looks)
    with jax.named_scope("link"):
        vec_real, vec_imag = link(coherence, WINDOWS)

    with jax.named_scope("note"):
        rows = jnp.concatenate([vec_real] + [vec_imag] * 4 + [vec_real] * 3, axis=0)
        turn[...] = rows.T
        lane = lane_iota((2 * n, 128))
        message = jnp.zeros((2 * n, 128), F32)
        for q in range(4):
            message = jnp.where((8 - lane // 16) % 4 == q, turn[pl.ds(q, 2 * n, stride=4), :], message)
        for d in range(n):
            note[d] = message[2 * d:2 * d + 2]

    def note_copy(k):
        to = lax.rem(me + k, n)
        return pltpu.make_async_remote_copy(
            src_ref=note.at[to], dst_ref=notes.at[me], send_sem=note_send.at[0], recv_sem=note_recv.at[k],
            device_id={"date": to}, device_id_type=MESH,
        )

    with jax.named_scope("notes"):
        for k in order:
            note_copy(k).start()
        notes[me] = note[me]
        pltpu.make_async_copy(send.at[0:n - 1], send.at[0:n - 1], send_sem.at[0]).wait()
        for k in order:
            source = lax.rem(me + n - k, n)
            pltpu.make_async_remote_copy(
                src_ref=note.at[source], dst_ref=notes.at[source], send_sem=note_send.at[0], recv_sem=note_recv.at[k],
                device_id={"date": source}, device_id_type=MESH,
            ).wait_recv()

    pltpu.make_async_copy(note.at[0:n - 1], note.at[0:n - 1], note_send.at[0]).wait()


def store(coherence, notes, coherence_out, linked_out, linked, sem):
    copies = [pltpu.make_async_copy(coherence.at[:, :, :, i], coherence_out.at[:, :, :, i], sem.at[i]) for i in range(WINDOWS)]
    for copy in copies:
        copy.start()
    lane = lane_iota((8, 128))
    for h in range(2):
        for half in range(2):
            tile = jnp.zeros((8, 128), F32)
            came = jnp.concatenate([notes[half * 8 + s, h:h + 1, :] for s in range(8)], axis=0)
            came = pltpu.roll(came, 0, 1, stride=16, stride_axis=0)
            for s in range(8):
                source = jnp.broadcast_to(came[s:s + 1], (8, 128))
                moved = pltpu.roll(source, 0, 1, stride=16, stride_axis=0)
                tile = jnp.where(lane // 16 == s, moved, tile)
            for c in range(2):
                linked[c, 4 * h:4 * h + 4, half * 128:half * 128 + 128] = tile[4 * c:4 * c + 4]
    copies.append(pltpu.make_async_copy(linked, linked_out, sem.at[WINDOWS]))
    copies[-1].start()
    for copy in copies:
        copy.wait()


def solution(mesh):
    n = mesh.shape["date"]

    def step(slc, usable):
        dates, windows = slc.shape[2], slc.shape[3]
        rows = 2 * slc.shape[1] * dates
        per_device = windows // n
        vmem, hbm = pl.BlockSpec(memory_space=pltpu.VMEM), pl.BlockSpec(memory_space=pl.ANY)
        coherence_shape, linked_shape = (2, 1, 1, per_device, n * dates, n * dates), (2, dates, windows)
        coherence, notes = pl.pallas_call(
            functools.partial(kernel, n),
            out_shape=(pltpu.VMEM(coherence_shape, BF16), pltpu.VMEM((n, 2, 128), F32)),
            in_specs=[hbm, hbm],
            out_specs=(vmem, vmem),
            scratch_shapes=[
                pltpu.VMEM(slc.shape, BF16),
                pltpu.VMEM(usable.shape, jnp.int32),
                pltpu.VMEM((windows // 128, rows, 128), F32),
                pltpu.VMEM((windows * dates, 128), F32),
                pltpu.VMEM((windows * dates // 2, 128), F32),
                pltpu.VMEM((n, TILES, dates, 128), BF16),
                pltpu.VMEM((TILES, n, dates, 128), BF16),
                pltpu.VMEM((128, 128), F32),
                pltpu.VMEM((n, 2, 128), F32),
                pltpu.SemaphoreType.DMA((LOADS, 3)),
                pltpu.SemaphoreType.DMA((1,)),
                pltpu.SemaphoreType.DMA((2, n)),
                pltpu.SemaphoreType.DMA((1,)),
                pltpu.SemaphoreType.DMA((n,)),
                pltpu.SemaphoreType.REGULAR,
                pltpu.SemaphoreType.REGULAR((n,)),
            ],
            compiler_params=pltpu.CompilerParams(collective_id=0, has_side_effects=True),
        )(slc, usable)
        return pl.pallas_call(
            store,
            out_shape=(jax.ShapeDtypeStruct(coherence_shape, BF16), jax.ShapeDtypeStruct(linked_shape, F32)),
            in_specs=[vmem, vmem],
            out_specs=(hbm, hbm),
            scratch_shapes=[pltpu.VMEM(linked_shape, F32), pltpu.SemaphoreType.DMA((WINDOWS + 1,))],
        )(pltpu.with_memory_space_constraint(coherence, pltpu.VMEM), pltpu.with_memory_space_constraint(notes, pltpu.VMEM))

    return jax.shard_map(
        step,
        mesh=mesh,
        in_specs=(
            P(None, None, "date", ("slab", "tile", "sub")),
            P(None, "date", ("slab", "tile", "sub")),
        ),
        out_specs=(
            P(None, ("slab", "tile", "sub"), "date", None, None, None),
            P(None, "date", ("slab", "tile", "sub")),
        ),
        check_vma=False,
    )
```

```python
import functools

import jax
import jax.numpy as jnp
from jax import lax
from jax.experimental import pallas as pl
from jax.experimental.pallas import tpu as pltpu
from jax.sharding import PartitionSpec as P

ITERS = 4
MESH = pl.DeviceIdType.MESH
F32, BF16 = jnp.float32, jnp.bfloat16
WINDOWS = 16
LATE = 3
LOADS = 5
CHUNKS = ((0, 13), (13, 12))
TILES = 25
REST = 12


def places(i):
    chunk, spot = divmod(i % 8, 4)
    return CHUNKS[chunk][0] + 4 * (i // 8) + spot, CHUNKS[chunk][0] + 8 + spot


def lane_iota(shape):
    return lax.broadcasted_iota(jnp.int32, shape, len(shape) - 1)


def pack(slc_ref, usable_ref, plane, split1, split2, send, loads, between, looks, dates, blocks):
    rows = looks * dates
    step = looks // LOADS

    def mask_step(l, carry):
        use = usable_ref[l].astype(F32)
        for c in range(2):
            masked = slc_ref[c, l].astype(F32) * use
            at = pl.ds(pl.multiple_of(c * rows + l * dates, 8), dates)
            for half in range(2):
                plane[half, at, :] = masked[:, half * 128:half * 128 + 128]
        return carry

    with jax.named_scope("mask"):
        for piece, copies in enumerate(loads):
            for copy in copies:
                copy.wait()
            lax.fori_loop(piece * step, piece * step + step, mask_step, 0, unroll=4)
    between()

    bit = (lane_iota((8, 8, 128)) // 8) % 2 == 1
    groups = [(c, r) for c in range(2) for r in range(4)]
    for half in range(2):

        def group(a, c, look, count):
            return plane[half, pl.ds(c * rows + look * dates + a, count, stride=dates), :]

        def date_step(a, carry):
            first = jnp.concatenate([group(a, c, 0, 64) for c in range(2)], axis=0)
            split1[pl.ds(half * 1024 + a, 128, stride=8), :] = first.T
            parts = []
            for c in range(2):
                for u in range(4):
                    rest = group(a, c, 64 + 8 * u, 8)
                    parts += [rest, rest]
            second = jnp.concatenate(parts, axis=0).T.reshape(8, 2, 8, 128)
            pairs = jnp.where(bit, second[:, 0], second[:, 1]).reshape(64, 128)
            split2[pl.ds(half * 512 + a, 64, stride=8), :] = pairs
            return carry

        lax.fori_loop(0, dates, date_step, 0, unroll=4)

        left = [plane[half, c * rows + (96 + r) * dates:c * rows + (97 + r) * dates, :] for c, r in groups]
        for b in range(8):
            tile = jnp.zeros((8, 128), F32)
            for g, part in enumerate(left):
                shift = (16 * (g - b)) % 128
                moved = pltpu.roll(part, shift, 1) if shift else part
                tile = jnp.where(lane_iota((8, 128)) // 16 == g, moved, tile)
            send[half * 8 + b, REST] = tile.astype(BF16)

    def out_step(b, carry):
        one = split1[pl.ds(pl.multiple_of(b * 128, 128), 128), :].reshape(16, 8, 128).astype(BF16)
        two = split2[pl.ds(pl.multiple_of(b * 64, 64), 64), :].reshape(8, 8, 128).astype(BF16)
        for chunk, (base, _) in enumerate(CHUNKS):
            send[b, base:base + 4] = one[4 * chunk:4 * chunk + 4]
            send[b, base + 4:base + 8] = one[8 + 4 * chunk:12 + 4 * chunk]
            send[b, base + 8:base + 12] = two[4 * chunk:4 * chunk + 4]
        return carry

    with jax.named_scope("cast"):
        lax.fori_loop(0, blocks, out_step, 0)


def gram(recv, coherence, i, looks):
    lane = lane_iota((128, 128))
    own, shared = places(i)
    one = recv[own].astype(F32).reshape(128, 128)
    pair = recv[shared].astype(F32).reshape(128, 128)
    rest = recv[REST].astype(F32).reshape(128, 128)
    in_pair = ((lane // 8) % 2 == 1) == (i < 8)
    two = jnp.where(in_pair, pair, jnp.where(lane % 16 == i, rest, 0.0))
    sign = jnp.where(lane < 64, 1.0, -1.0)
    plain = jnp.concatenate([one, two], axis=1).astype(BF16)
    turned = jnp.concatenate([pltpu.roll(one, 64, 1) * sign, pltpu.roll(two, 64, 1) * sign], axis=1).astype(BF16)
    both = jnp.concatenate([plain, turned], axis=0)
    cross = lax.dot_general(both, plain, (((1,), (1,)), ((), ())), preferred_element_type=F32)
    real, imag = cross[:128], cross[128:]
    eye = lax.broadcasted_iota(jnp.int32, (128, 128), 0) == lane
    diagonal = jnp.where(eye, real, 0.0)
    column = lax.rsqrt(jnp.sum(diagonal, axis=1, keepdims=True) * (1.0 / looks) + 1e-05)
    row = lax.rsqrt(jnp.sum(diagonal, axis=0, keepdims=True) * (1.0 / looks) + 1e-05)
    factor = column * row * (1.0 / looks)
    coherence[0, 0, 0, i] = (real * factor).astype(BF16)
    coherence[1, 0, 0, i] = (imag * factor).astype(BF16)


def link(coherence, members):
    windows = len(members)
    row = lax.broadcasted_iota(jnp.int32, (4 * windows, 256), 0) % windows
    real, imag = jnp.ones((windows, 128), F32), jnp.zeros((windows, 128), F32)
    scale = None
    for step in range(ITERS):
        high_real, high_imag = real.astype(BF16).astype(F32), imag.astype(BF16).astype(F32)
        low_real, low_imag = real - high_real, imag - high_imag
        lhs = jnp.concatenate(
            [
                jnp.concatenate([high_real, high_imag], axis=1),
                jnp.concatenate([low_real, low_imag], axis=1),
                jnp.concatenate([high_imag, -high_real], axis=1),
                jnp.concatenate([low_imag, -low_real], axis=1),
            ],
            axis=0,
        )
        total = jnp.zeros((4 * windows, 128), F32)
        for w, i in enumerate(members):
            stacked = jnp.concatenate([coherence[0, 0, 0, i], coherence[1, 0, 0, i]], axis=0)
            total += jnp.dot(jnp.where(row == w, lhs, 0.0).astype(BF16), stacked, preferred_element_type=F32)
        real = total[:windows] + total[windows:2 * windows]
        imag = total[2 * windows:3 * windows] + total[3 * windows:]
        if scale is not None:
            real, imag = real * scale, imag * scale
        scale = lax.rsqrt(jnp.sum(real * real + imag * imag, axis=1, keepdims=True) * (1.0 / 128) + 1e-05)
    return real * scale, imag * scale


def kernel(
    n, slc_hbm, usable_hbm, coherence, notes, slc_ref, usable_ref, plane, split1, split2, send, recv, turn, note,
    load_sem, send_sem, recv_sem, note_send, note_recv, known_sem,
):
    looks, dates = slc_ref.shape[1], slc_ref.shape[2]
    me = lax.axis_index("date")
    barrier = pltpu.get_barrier_semaphore()
    order = []
    for k in range(n // 2, 0, -1):
        order += [k] if 2 * k == n else [k, n - k]
    loads = []
    for piece in range(LOADS):
        part = pl.ds(piece * (looks // LOADS), looks // LOADS)
        loads.append([
            pltpu.make_async_copy(slc_hbm.at[:, part], slc_ref.at[:, part], load_sem.at[piece, 0]),
            pltpu.make_async_copy(usable_hbm.at[part], usable_ref.at[part], load_sem.at[piece, 1]),
        ])
        for copy in loads[-1]:
            copy.start()

    first = me == 0

    def rank_of(z):
        if isinstance(z, int):
            return n - 2 if z in (0, n - 1) else z - 1
        return jnp.where((z == 0) | (z == n - 1), n - 2, z - 1)

    rank = rank_of(me)

    def enter():
        @pl.when(rank > 0)
        def _():
            pl.semaphore_wait(barrier, 1)

        @pl.when(rank < n - 2)
        def _():
            pl.semaphore_signal(barrier, inc=1, device_id={"date": me + 1}, device_id_type=MESH)

        @pl.when(me == n - 2)
        def _():
            pl.semaphore_signal(barrier, inc=1, device_id={"date": 0}, device_id_type=MESH)

        for k in order:
            to = lax.rem(me + k, n)

            @pl.when(rank_of(to) < rank)
            def _():
                pl.semaphore_signal(known_sem.at[me], inc=1, device_id={"date": to}, device_id_type=MESH)

    pl.when(me > 0)(enter)
    pack(slc_ref, usable_ref, plane, split1, split2, send, loads, lambda: pl.when(first)(enter), looks, dates, n)

    def sample_copy(chunk, to, source):
        tiles = pl.ds(*CHUNKS[chunk])
        return pltpu.make_async_remote_copy(
            src_ref=send.at[to, tiles], dst_ref=recv.at[tiles, source], send_sem=send_sem.at[0], recv_sem=recv_sem.at[chunk, source],
            device_id={"date": to}, device_id_type=MESH,
        )

    def send_lower(chunk):
        for k in order:
            to = lax.rem(me + k, n)

            @pl.when(rank_of(to) < rank)
            def _():
                sample_copy(chunk, to, me).start()

    late = n - LATE
    entry = [*range(1, n - 1), 0, n - 1]
    with jax.named_scope("start"):
        send_lower(0)
        pl.when(rank < late)(lambda: send_lower(1))
        recv[:, me] = send[me]
        for place, z in enumerate(entry):

            @pl.when(rank < rank_of(z))
            def _():
                pl.semaphore_wait(known_sem.at[z], 1)
                for chunk in range(2 if place < late else 1):
                    sample_copy(chunk, z, me).start()

        @pl.when(me == n - 2)
        def _():
            pl.semaphore_signal(known_sem.at[0], inc=1, device_id={"date": n - 1}, device_id_type=MESH)
            pl.semaphore_signal(known_sem.at[n - 1], inc=1, device_id={"date": 0}, device_id_type=MESH)

        pl.when(rank >= late)(lambda: send_lower(1))
        for z in entry[late:]:

            @pl.when(rank < rank_of(z))
            def _():
                sample_copy(1, z, me).start()

        for one, other in ((0, n - 1), (n - 1, 0)):

            @pl.when(me == one)
            def _():
                pl.semaphore_wait(known_sem.at[other], 1)
                for chunk in range(2):
                    sample_copy(chunk, other, me).start()

    linked = []
    for chunk in range(2):
        with jax.named_scope("receive"):
            for k in order:
                source = lax.rem(me + n - k, n)
                sample_copy(chunk, source, source).wait_recv()
        members = [i for i in range(WINDOWS) if (i % 8) // 4 == chunk]
        with jax.named_scope("gram"):
            for i in members:
                gram(recv, coherence, i, looks)
        with jax.named_scope("link"):
            linked.append(link(coherence, members))
    vec_real, vec_imag = [
        jnp.concatenate([linked[0][c][:4], linked[1][c][:4], linked[0][c][4:], linked[1][c][4:]], axis=0) for c in range(2)
    ]

    with jax.named_scope("note"):
        rows = jnp.concatenate([vec_real] + [vec_imag] * 4 + [vec_real] * 3, axis=0)
        turn[...] = rows.T
        lane = lane_iota((2 * n, 128))
        message = jnp.zeros((2 * n, 128), F32)
        for q in range(4):
            message = jnp.where((8 - lane // 16) % 4 == q, turn[pl.ds(q, 2 * n, stride=4), :], message)
        for d in range(n):
            note[d] = message[2 * d:2 * d + 2]

    def note_copy(k):
        to = lax.rem(me + k, n)
        return pltpu.make_async_remote_copy(
            src_ref=note.at[to], dst_ref=notes.at[me], send_sem=note_send.at[0], recv_sem=note_recv.at[k],
            device_id={"date": to}, device_id_type=MESH,
        )

    with jax.named_scope("notes"):
        for k in order:
            note_copy(k).start()
        notes[me] = note[me]
        pltpu.make_async_copy(send.at[0:n - 1], send.at[0:n - 1], send_sem.at[0]).wait()
        for k in order:
            source = lax.rem(me + n - k, n)
            pltpu.make_async_remote_copy(
                src_ref=note.at[source], dst_ref=notes.at[source], send_sem=note_send.at[0], recv_sem=note_recv.at[k],
                device_id={"date": source}, device_id_type=MESH,
            ).wait_recv()

    pltpu.make_async_copy(note.at[0:n - 1], note.at[0:n - 1], note_send.at[0]).wait()


def store(coherence, notes, coherence_out, linked_out, linked, sem):
    copies = [pltpu.make_async_copy(coherence.at[:, :, :, i], coherence_out.at[:, :, :, i], sem.at[i]) for i in range(WINDOWS)]
    for copy in copies:
        copy.start()
    lane = lane_iota((8, 128))
    for h in range(2):
        for half in range(2):
            tile = jnp.zeros((8, 128), F32)
            came = jnp.concatenate([notes[half * 8 + s, h:h + 1, :] for s in range(8)], axis=0)
            came = pltpu.roll(came, 0, 1, stride=16, stride_axis=0)
            for s in range(8):
                source = jnp.broadcast_to(came[s:s + 1], (8, 128))
                moved = pltpu.roll(source, 0, 1, stride=16, stride_axis=0)
                tile = jnp.where(lane // 16 == s, moved, tile)
            for c in range(2):
                linked[c, 4 * h:4 * h + 4, half * 128:half * 128 + 128] = tile[4 * c:4 * c + 4]
    copies.append(pltpu.make_async_copy(linked, linked_out, sem.at[WINDOWS]))
    copies[-1].start()
    for copy in copies:
        copy.wait()


def solution(mesh):
    n = mesh.shape["date"]

    def step(slc, usable):
        dates, windows = slc.shape[2], slc.shape[3]
        rows = 2 * slc.shape[1] * dates
        per_device = windows // n
        vmem, hbm = pl.BlockSpec(memory_space=pltpu.VMEM), pl.BlockSpec(memory_space=pl.ANY)
        coherence_shape, linked_shape = (2, 1, 1, per_device, n * dates, n * dates), (2, dates, windows)
        coherence, notes = pl.pallas_call(
            functools.partial(kernel, n),
            out_shape=(pltpu.VMEM(coherence_shape, BF16), pltpu.VMEM((n, 2, 128), F32)),
            in_specs=[hbm, hbm],
            out_specs=(vmem, vmem),
            scratch_shapes=[
                pltpu.VMEM(slc.shape, BF16),
                pltpu.VMEM(usable.shape, jnp.int32),
                pltpu.VMEM((windows // 128, rows, 128), F32),
                pltpu.VMEM((windows * dates, 128), F32),
                pltpu.VMEM((windows * dates // 2, 128), F32),
                pltpu.VMEM((n, TILES, dates, 128), BF16),
                pltpu.VMEM((TILES, n, dates, 128), BF16),
                pltpu.VMEM((128, 128), F32),
                pltpu.VMEM((n, 2, 128), F32),
                pltpu.SemaphoreType.DMA((LOADS, 2)),
                pltpu.SemaphoreType.DMA((1,)),
                pltpu.SemaphoreType.DMA((2, n)),
                pltpu.SemaphoreType.DMA((1,)),
                pltpu.SemaphoreType.DMA((n,)),
                pltpu.SemaphoreType.REGULAR((n,)),
            ],
            compiler_params=pltpu.CompilerParams(collective_id=0, has_side_effects=True),
        )(slc, usable)
        return pl.pallas_call(
            store,
            out_shape=(jax.ShapeDtypeStruct(coherence_shape, BF16), jax.ShapeDtypeStruct(linked_shape, F32)),
            in_specs=[vmem, vmem],
            out_specs=(hbm, hbm),
            scratch_shapes=[pltpu.VMEM(linked_shape, F32), pltpu.SemaphoreType.DMA((WINDOWS + 1,))],
        )(pltpu.with_memory_space_constraint(coherence, pltpu.VMEM), pltpu.with_memory_space_constraint(notes, pltpu.VMEM))

    return jax.shard_map(
        step,
        mesh=mesh,
        in_specs=(
            P(None, None, "date", ("slab", "tile", "sub")),
            P(None, "date", ("slab", "tile", "sub")),
        ),
        out_specs=(
            P(None, ("slab", "tile", "sub"), "date", None, None, None),
            P(None, "date", ("slab", "tile", "sub")),
        ),
        check_vma=False,
    )
```

```python
import functools

import jax
import jax.numpy as jnp
from jax import lax
from jax.experimental import pallas as pl
from jax.experimental.pallas import tpu as pltpu
from jax.sharding import PartitionSpec as P

ITERS = 4
MESH = pl.DeviceIdType.MESH
F32, BF16 = jnp.float32, jnp.bfloat16
WINDOWS = 16
LATE = 3
SPLIT = 4
LOADS = 5
PAIRS = (SPLIT, 8 - SPLIT)
REST = 3 * SPLIT
TILES = 25
CHUNKS = ((0, REST + 1), (REST + 1, TILES - REST - 1))


def places(i):
    chunk = int(i % 8 >= SPLIT)
    spot = CHUNKS[chunk][0] + i % 8 - chunk * SPLIT
    return chunk, spot + PAIRS[chunk] * (i // 8), spot + 2 * PAIRS[chunk]


def lane_iota(shape):
    return lax.broadcasted_iota(jnp.int32, shape, len(shape) - 1)


def pack(slc_ref, usable_ref, plane, split1, split2, send, loads, between, ready, looks, dates):
    rows = looks * dates
    step = looks // LOADS

    def mask_step(l, carry):
        use = usable_ref[l].astype(F32)
        for c in range(2):
            masked = slc_ref[c, l].astype(F32) * use
            at = pl.ds(pl.multiple_of(c * rows + l * dates, 8), dates)
            for half in range(2):
                plane[half, at, :] = masked[:, half * 128:half * 128 + 128]
        return carry

    with jax.named_scope("mask"):
        for piece, copies in enumerate(loads):
            for copy in copies:
                copy.wait()
            lax.fori_loop(piece * step, piece * step + step, mask_step, 0, unroll=20)
    between()

    def out_step(b, carry):
        one = split1[pl.ds(pl.multiple_of(b * 128, 128), 128), :].reshape(16, 8, 128).astype(BF16)
        two = split2[pl.ds(pl.multiple_of(b * 64, 64), 64), :].reshape(8, 8, 128).astype(BF16)
        for (base, _), count, at in zip(CHUNKS, PAIRS, (0, SPLIT)):
            send[b, base:base + count] = one[at:at + count]
            send[b, base + count:base + 2 * count] = one[8 + at:8 + at + count]
            send[b, base + 2 * count:base + 3 * count] = two[at:at + count]
        return carry

    bit = (lane_iota((8, 8, 128)) // 8) % 2 == 1
    groups = [(c, r) for c in range(2) for r in range(4)]
    for half in range(2):

        def group(a, c, look, count):
            return plane[half, pl.ds(c * rows + look * dates + a, count, stride=dates), :]

        def date_step(a, carry):
            first = jnp.concatenate([group(a, c, 0, 64) for c in range(2)], axis=0)
            split1[pl.ds(half * 1024 + a, 128, stride=8), :] = first.T
            parts = []
            for c in range(2):
                for u in range(4):
                    rest = group(a, c, 64 + 8 * u, 8)
                    parts += [rest, rest]
            second = jnp.concatenate(parts, axis=0).T.reshape(8, 2, 8, 128)
            pairs = jnp.where(bit, second[:, 0], second[:, 1]).reshape(64, 128)
            split2[pl.ds(half * 512 + a, 64, stride=8), :] = pairs
            return carry

        lax.fori_loop(0, dates, date_step, 0, unroll=8)

        left = [plane[half, c * rows + (96 + r) * dates:c * rows + (97 + r) * dates, :] for c, r in groups]
        for b in range(8):
            tile = jnp.zeros((8, 128), F32)
            for g, part in enumerate(left):
                shift = (16 * (g - b)) % 128
                moved = pltpu.roll(part, shift, 1) if shift else part
                tile = jnp.where(lane_iota((8, 128)) // 16 == g, moved, tile)
            send[half * 8 + b, REST] = tile.astype(BF16)

        lax.fori_loop(8 * half, 8 * half + 8, out_step, 0)
        ready(half)


def gram(recv, coherence, i, looks):
    lane = lane_iota((128, 128))
    _, own, shared = places(i)
    one = recv[own].astype(F32).reshape(128, 128)
    pair = recv[shared].astype(F32).reshape(128, 128)
    rest = recv[REST].astype(F32).reshape(128, 128)
    in_pair = ((lane // 8) % 2 == 1) == (i < 8)
    two = jnp.where(in_pair, pair, jnp.where(lane % 16 == i, rest, 0.0))
    plain = jnp.concatenate([one, two], axis=1).astype(BF16)
    turned = jnp.concatenate([one.T, two.T], axis=0)
    swapped = jnp.concatenate([-turned[64:128], turned[:64], -turned[192:], turned[128:192]], axis=0)
    cross = jnp.dot(plain, jnp.concatenate([turned, swapped], axis=1).astype(BF16), preferred_element_type=F32)
    real, imag = cross[:, :128], cross[:, 128:]
    eye = lax.broadcasted_iota(jnp.int32, (128, 128), 0) == lane
    diagonal = jnp.where(eye, real, 0.0)
    column = lax.rsqrt(jnp.sum(diagonal, axis=1, keepdims=True) * (1.0 / looks) + 1e-05)
    row = lax.rsqrt(jnp.sum(diagonal, axis=0, keepdims=True) * (1.0 / looks) + 1e-05)
    factor = column * row * (1.0 / looks)
    coherence[0, 0, 0, i] = (real * factor).astype(BF16)
    coherence[1, 0, 0, i] = (imag * factor).astype(BF16)


def link(coherence, members):
    windows = -(-len(members) // 8) * 8
    row = lax.broadcasted_iota(jnp.int32, (4 * windows, 128), 0) % windows
    real, imag = jnp.ones((windows, 128), F32), jnp.zeros((windows, 128), F32)
    scale = None
    for step in range(ITERS):
        high_real, high_imag = real.astype(BF16).astype(F32), imag.astype(BF16).astype(F32)
        low_real, low_imag = real - high_real, imag - high_imag
        lhs = jnp.concatenate(
            [
                jnp.concatenate([high_real, high_imag], axis=1),
                jnp.concatenate([low_real, low_imag], axis=1),
                jnp.concatenate([high_imag, -high_real], axis=1),
                jnp.concatenate([low_imag, -low_real], axis=1),
            ],
            axis=0,
        )
        lhs = lhs.astype(BF16)
        total = jnp.zeros((4 * windows, 128), F32)
        for w in range(0, len(members), 2):
            matrices = jnp.concatenate(
                [jnp.concatenate([coherence[c, 0, 0, i] for c in range(2)], axis=0) for i in members[w:w + 2]], axis=1
            )
            product = jnp.dot(lhs, matrices, preferred_element_type=F32)
            total = jnp.where(row == w, product[:, :128], jnp.where(row == w + 1, product[:, 128:], total))
        real = total[:windows] + total[windows:2 * windows]
        imag = total[2 * windows:3 * windows] + total[3 * windows:]
        if scale is not None:
            real, imag = real * scale, imag * scale
        scale = lax.rsqrt(jnp.sum(real * real + imag * imag, axis=1, keepdims=True) * (1.0 / 128) + 1e-05)
    return real * scale, imag * scale


def kernel(
    n, slc_hbm, usable_hbm, coherence, notes, slc_ref, usable_ref, plane, split1, split2, send, recv, turn, note,
    load_sem, send_sem, recv_sem, note_send, note_recv, known_sem,
):
    looks, dates = slc_ref.shape[1], slc_ref.shape[2]
    me = lax.axis_index("date")
    barrier = pltpu.get_barrier_semaphore()
    order = []
    for k in range(n // 2, 0, -1):
        order += [k] if 2 * k == n else [k, n - k]
    loads = []
    for piece in range(LOADS):
        part = pl.ds(piece * (looks // LOADS), looks // LOADS)
        loads.append([
            pltpu.make_async_copy(slc_hbm.at[:, part], slc_ref.at[:, part], load_sem.at[piece, 0]),
            pltpu.make_async_copy(usable_hbm.at[part], usable_ref.at[part], load_sem.at[piece, 1]),
        ])
        for copy in loads[-1]:
            copy.start()

    first = me == 0

    def rank_of(z):
        if isinstance(z, int):
            return n - 2 if z in (0, n - 1) else z - 1
        return jnp.where((z == 0) | (z == n - 1), n - 2, z - 1)

    rank = rank_of(me)

    def enter():
        @pl.when(rank > 0)
        def _():
            pl.semaphore_wait(barrier, 1)

        @pl.when(rank < n - 2)
        def _():
            pl.semaphore_signal(barrier, inc=1, device_id={"date": me + 1}, device_id_type=MESH)

        @pl.when(me == n - 2)
        def _():
            pl.semaphore_signal(barrier, inc=1, device_id={"date": 0}, device_id_type=MESH)

        for k in order:
            to = lax.rem(me + k, n)

            @pl.when(rank_of(to) < rank)
            def _():
                pl.semaphore_signal(known_sem.at[me], inc=1, device_id={"date": to}, device_id_type=MESH)

    def sample_copy(chunk, to, source):
        tiles = pl.ds(*CHUNKS[chunk])
        return pltpu.make_async_remote_copy(
            src_ref=send.at[to, tiles], dst_ref=recv.at[tiles, source], send_sem=send_sem.at[0], recv_sem=recv_sem.at[chunk, source],
            device_id={"date": to}, device_id_type=MESH,
        )

    def ready(half):
        for k in order:
            to = lax.rem(me + k, n)

            @pl.when((rank_of(to) < rank) & (to // (n // 2) == half))
            def _():
                sample_copy(0, to, me).start()

    pl.when(me > 0)(enter)
    pack(slc_ref, usable_ref, plane, split1, split2, send, loads, lambda: pl.when(first)(enter), ready, looks, dates)

    def send_lower():
        for k in order:
            to = lax.rem(me + k, n)

            @pl.when(rank_of(to) < rank)
            def _():
                sample_copy(1, to, me).start()

    late = n - LATE
    entry = [*range(1, n - 1), 0, n - 1]
    with jax.named_scope("start"):
        pl.when(rank < late)(send_lower)
        recv[:, me] = send[me]
        for place, z in enumerate(entry):

            @pl.when(rank < rank_of(z))
            def _():
                pl.semaphore_wait(known_sem.at[z], 1)
                for chunk in range(2 if place < late else 1):
                    sample_copy(chunk, z, me).start()

        @pl.when(me == n - 2)
        def _():
            pl.semaphore_signal(known_sem.at[0], inc=1, device_id={"date": n - 1}, device_id_type=MESH)
            pl.semaphore_signal(known_sem.at[n - 1], inc=1, device_id={"date": 0}, device_id_type=MESH)

        pl.when(rank >= late)(send_lower)
        for z in entry[late:]:

            @pl.when(rank < rank_of(z))
            def _():
                sample_copy(1, z, me).start()

        for one, other in ((0, n - 1), (n - 1, 0)):

            @pl.when(me == one)
            def _():
                pl.semaphore_wait(known_sem.at[other], 1)
                for chunk in range(2):
                    sample_copy(chunk, other, me).start()

    linked = []
    for chunk in range(2):
        with jax.named_scope("receive"):
            for k in order:
                source = lax.rem(me + n - k, n)
                sample_copy(chunk, source, source).wait_recv()
        members = [i for i in range(WINDOWS) if places(i)[0] == chunk]
        with jax.named_scope("gram"):
            for i in members:
                gram(recv, coherence, i, looks)
        with jax.named_scope("link"):
            linked.append(link(coherence, members))
    vec_real, vec_imag = [
        jnp.concatenate([linked[chunk][c][half * PAIRS[chunk]:][:PAIRS[chunk]] for half in range(2) for chunk in range(2)], axis=0)
        for c in range(2)
    ]

    with jax.named_scope("note"):
        rows = jnp.concatenate([vec_real] + [vec_imag] * 4 + [vec_real] * 3, axis=0)
        turn[0:128] = rows.T
        lane = lane_iota((2 * n, 128))
        message = jnp.zeros((2 * n, 128), F32)
        for q in range(4):
            message = jnp.where((8 - lane // 16) % 4 == q, turn[pl.ds(q, 2 * n, stride=4), :], message)
        for d in range(n):
            note[d] = message[2 * d:2 * d + 2]

    def note_copy(k):
        to = lax.rem(me + k, n)
        return pltpu.make_async_remote_copy(
            src_ref=note.at[to], dst_ref=notes.at[me], send_sem=note_send.at[0], recv_sem=note_recv.at[k],
            device_id={"date": to}, device_id_type=MESH,
        )

    with jax.named_scope("notes"):
        for k in order:
            note_copy(k).start()
        notes[me] = note[me]
        pltpu.make_async_copy(send.at[0:n - 1], send.at[0:n - 1], send_sem.at[0]).wait()
        pltpu.make_async_copy(note.at[0:n - 1], note.at[0:n - 1], note_send.at[0]).wait()
        for k in order:
            source = lax.rem(me + n - k, n)
            pltpu.make_async_remote_copy(
                src_ref=note.at[source], dst_ref=notes.at[source], send_sem=note_send.at[0], recv_sem=note_recv.at[k],
                device_id={"date": source}, device_id_type=MESH,
            ).wait_recv()


def store(coherence, notes, coherence_out, linked_out, linked, sem):
    copies = [pltpu.make_async_copy(coherence.at[:, :, :, i], coherence_out.at[:, :, :, i], sem.at[i]) for i in range(WINDOWS)]
    for copy in copies:
        copy.start()
    lane = lane_iota((8, 128))
    for h in range(2):
        for half in range(2):
            tile = jnp.zeros((8, 128), F32)
            came = jnp.concatenate([notes[half * 8 + s, h:h + 1, :] for s in range(8)], axis=0)
            came = pltpu.roll(came, 0, 1, stride=16, stride_axis=0)
            for s in range(8):
                source = jnp.broadcast_to(came[s:s + 1], (8, 128))
                moved = pltpu.roll(source, 0, 1, stride=16, stride_axis=0)
                tile = jnp.where(lane // 16 == s, moved, tile)
            for c in range(2):
                linked[c, 4 * h:4 * h + 4, half * 128:half * 128 + 128] = tile[4 * c:4 * c + 4]
    copies.append(pltpu.make_async_copy(linked, linked_out, sem.at[WINDOWS]))
    copies[-1].start()
    for copy in copies:
        copy.wait()


def solution(mesh):
    n = mesh.shape["date"]

    def step(slc, usable):
        dates, windows = slc.shape[2], slc.shape[3]
        rows = 2 * slc.shape[1] * dates
        per_device = windows // n
        vmem, hbm = pl.BlockSpec(memory_space=pltpu.VMEM), pl.BlockSpec(memory_space=pl.ANY)
        coherence_shape, linked_shape = (2, 1, 1, per_device, n * dates, n * dates), (2, dates, windows)
        coherence, notes = pl.pallas_call(
            functools.partial(kernel, n),
            out_shape=(pltpu.VMEM(coherence_shape, BF16), pltpu.VMEM((n, 2, 128), F32)),
            in_specs=[hbm, hbm],
            out_specs=(vmem, vmem),
            scratch_shapes=[
                pltpu.VMEM(slc.shape, BF16),
                pltpu.VMEM(usable.shape, jnp.int32),
                pltpu.VMEM((windows // 128, rows + 8, 128), F32),
                pltpu.VMEM((windows * dates + 8, 128), F32),
                pltpu.VMEM((windows * dates // 2 + 8, 128), F32),
                pltpu.VMEM((n, TILES, dates, 128), BF16),
                pltpu.VMEM((TILES, n, dates, 128), BF16),
                pltpu.VMEM((136, 128), F32),
                pltpu.VMEM((n, 2, 128), F32),
                pltpu.SemaphoreType.DMA((LOADS, 2)),
                pltpu.SemaphoreType.DMA((1,)),
                pltpu.SemaphoreType.DMA((2, n)),
                pltpu.SemaphoreType.DMA((1,)),
                pltpu.SemaphoreType.DMA((n,)),
                pltpu.SemaphoreType.REGULAR((n,)),
            ],
            compiler_params=pltpu.CompilerParams(collective_id=0, has_side_effects=True),
        )(slc, usable)
        return pl.pallas_call(
            store,
            out_shape=(jax.ShapeDtypeStruct(coherence_shape, BF16), jax.ShapeDtypeStruct(linked_shape, F32)),
            in_specs=[vmem, vmem],
            out_specs=(hbm, hbm),
            scratch_shapes=[pltpu.VMEM(linked_shape, F32), pltpu.SemaphoreType.DMA((WINDOWS + 1,))],
        )(pltpu.with_memory_space_constraint(coherence, pltpu.VMEM), pltpu.with_memory_space_constraint(notes, pltpu.VMEM))

    return jax.shard_map(
        step,
        mesh=mesh,
        in_specs=(
            P(None, None, "date", ("slab", "tile", "sub")),
            P(None, "date", ("slab", "tile", "sub")),
        ),
        out_specs=(
            P(None, ("slab", "tile", "sub"), "date", None, None, None),
            P(None, "date", ("slab", "tile", "sub")),
        ),
        check_vma=False,
    )
```

```python
import functools

import jax
import jax.numpy as jnp
from jax import lax
from jax.experimental import pallas as pl
from jax.experimental.pallas import tpu as pltpu
from jax.sharding import PartitionSpec as P

ITERS = 4
MESH = pl.DeviceIdType.MESH
F32, BF16 = jnp.float32, jnp.bfloat16
WINDOWS = 16
LATE = 3
SPLIT = 4
LOADS = 5
PAIRS = (SPLIT, 8 - SPLIT)
REST = 3 * SPLIT
TILES = 25
CHUNKS = ((0, REST + 1), (REST + 1, TILES - REST - 1))


def places(i):
    chunk = int(i % 8 >= SPLIT)
    spot = CHUNKS[chunk][0] + i % 8 - chunk * SPLIT
    return chunk, spot + PAIRS[chunk] * (i // 8), spot + 2 * PAIRS[chunk]


def lane_iota(shape):
    return lax.broadcasted_iota(jnp.int32, shape, len(shape) - 1)


def pack(slc_ref, usable_ref, plane, split1, split2, send, loads, between, ready, looks, dates):
    rows = looks * dates
    step = looks // LOADS

    def mask_step(l, carry):
        use = usable_ref[l].astype(F32)
        for c in range(2):
            masked = slc_ref[c, l].astype(F32) * use
            at = pl.ds(pl.multiple_of(c * rows + l * dates, 8), dates)
            for half in range(2):
                plane[half, at, :] = masked[:, half * 128:half * 128 + 128]
        return carry

    with jax.named_scope("mask"):
        for piece, copies in enumerate(loads):
            for copy in copies:
                copy.wait()
            lax.fori_loop(piece * step, piece * step + step, mask_step, 0, unroll=20)
    between()

    def out_step(b, carry):
        one = split1[pl.ds(pl.multiple_of(b * 128, 128), 128), :].reshape(16, 8, 128).astype(BF16)
        two = split2[pl.ds(pl.multiple_of(b * 64, 64), 64), :].reshape(8, 8, 128).astype(BF16)
        for (base, _), count, at in zip(CHUNKS, PAIRS, (0, SPLIT)):
            send[b, base:base + count] = one[at:at + count]
            send[b, base + count:base + 2 * count] = one[8 + at:8 + at + count]
            send[b, base + 2 * count:base + 3 * count] = two[at:at + count]
        return carry

    bit = (lane_iota((8, 8, 128)) // 8) % 2 == 1
    groups = [(c, r) for c in range(2) for r in range(4)]
    for half in range(2):

        def group(a, c, look, count):
            return plane[half, pl.ds(c * rows + look * dates + a, count, stride=dates), :]

        def date_step(a, carry):
            first = jnp.concatenate([group(a, c, 0, 64) for c in range(2)], axis=0)
            split1[pl.ds(half * 1024 + a, 128, stride=8), :] = first.T
            parts = []
            for c in range(2):
                for u in range(4):
                    rest = group(a, c, 64 + 8 * u, 8)
                    parts += [rest, rest]
            second = jnp.concatenate(parts, axis=0).T.reshape(8, 2, 8, 128)
            pairs = jnp.where(bit, second[:, 0], second[:, 1]).reshape(64, 128)
            split2[pl.ds(half * 512 + a, 64, stride=8), :] = pairs
            return carry

        lax.fori_loop(0, dates, date_step, 0, unroll=8)

        left = [plane[half, c * rows + (96 + r) * dates:c * rows + (97 + r) * dates, :] for c, r in groups]
        for b in range(8):
            tile = jnp.zeros((8, 128), F32)
            for g, part in enumerate(left):
                shift = (16 * (g - b)) % 128
                moved = pltpu.roll(part, shift, 1) if shift else part
                tile = jnp.where(lane_iota((8, 128)) // 16 == g, moved, tile)
            send[half * 8 + b, REST] = tile.astype(BF16)

        lax.fori_loop(8 * half, 8 * half + 8, out_step, 0)
        ready(half)


def gram(recv, coherence, i, looks):
    lane = lane_iota((128, 128))
    _, own, shared = places(i)
    one = recv[own].astype(F32).reshape(128, 128)
    pair = recv[shared].astype(F32).reshape(128, 128)
    rest = recv[REST].astype(F32).reshape(128, 128)
    in_pair = ((lane // 8) % 2 == 1) == (i < 8)
    two = jnp.where(in_pair, pair, jnp.where(lane % 16 == i, rest, 0.0))
    plain = jnp.concatenate([one, two], axis=1).astype(BF16)
    turned = jnp.concatenate([one.T, two.T], axis=0)
    swapped = jnp.concatenate([-turned[64:128], turned[:64], -turned[192:], turned[128:192]], axis=0)
    cross = jnp.dot(plain, jnp.concatenate([turned, swapped], axis=1).astype(BF16), preferred_element_type=F32)
    real, imag = cross[:, :128], cross[:, 128:]
    eye = lax.broadcasted_iota(jnp.int32, (128, 128), 0) == lane
    diagonal = jnp.where(eye, real, 0.0)
    column = lax.rsqrt(jnp.sum(diagonal, axis=1, keepdims=True) * (1.0 / looks) + 1e-05)
    row = lax.rsqrt(jnp.sum(diagonal, axis=0, keepdims=True) * (1.0 / looks) + 1e-05)
    factor = column * row * (1.0 / looks)
    rounded = [(real * factor).astype(BF16), (imag * factor).astype(BF16)]
    for c in range(2):
        coherence[c, 0, 0, i] = rounded[c]
    return [jnp.sum(part.astype(F32), axis=0, keepdims=True) for part in rounded]


def link(coherence, members, sums):
    windows = -(-len(members) // 8) * 8
    row = lax.broadcasted_iota(jnp.int32, (4 * windows, 128), 0) % windows
    assert windows == len(members)
    real = jnp.concatenate([pair[0] for pair in sums], axis=0)
    imag = -jnp.concatenate([pair[1] for pair in sums], axis=0)
    scale = lax.rsqrt(jnp.sum(real * real + imag * imag, axis=1, keepdims=True) * (1.0 / 128) + 1e-05)
    for step in range(1, ITERS):
        high_real, high_imag = real.astype(BF16).astype(F32), imag.astype(BF16).astype(F32)
        low_real, low_imag = real - high_real, imag - high_imag
        lhs = jnp.concatenate(
            [
                jnp.concatenate([high_real, high_imag], axis=1),
                jnp.concatenate([low_real, low_imag], axis=1),
                jnp.concatenate([high_imag, -high_real], axis=1),
                jnp.concatenate([low_imag, -low_real], axis=1),
            ],
            axis=0,
        )
        lhs = lhs.astype(BF16)
        total = jnp.zeros((4 * windows, 128), F32)
        for w in range(0, len(members), 2):
            matrices = jnp.concatenate(
                [jnp.concatenate([coherence[c, 0, 0, i] for c in range(2)], axis=0) for i in members[w:w + 2]], axis=1
            )
            product = jnp.dot(lhs, matrices, preferred_element_type=F32)
            total = jnp.where(row == w, product[:, :128], jnp.where(row == w + 1, product[:, 128:], total))
        real = total[:windows] + total[windows:2 * windows]
        imag = total[2 * windows:3 * windows] + total[3 * windows:]
        real, imag = real * scale, imag * scale
        scale = lax.rsqrt(jnp.sum(real * real + imag * imag, axis=1, keepdims=True) * (1.0 / 128) + 1e-05)
    return real * scale, imag * scale


def kernel(
    n, slc_hbm, usable_hbm, coherence, notes, slc_ref, usable_ref, plane, split1, split2, send, recv, turn, note,
    load_sem, send_sem, recv_sem, note_send, note_recv, known_sem,
):
    looks, dates = slc_ref.shape[1], slc_ref.shape[2]
    me = lax.axis_index("date")
    barrier = pltpu.get_barrier_semaphore()
    order = []
    for k in range(n // 2, 0, -1):
        order += [k] if 2 * k == n else [k, n - k]
    loads = []
    for piece in range(LOADS):
        part = pl.ds(piece * (looks // LOADS), looks // LOADS)
        loads.append([
            pltpu.make_async_copy(slc_hbm.at[:, part], slc_ref.at[:, part], load_sem.at[piece, 0]),
            pltpu.make_async_copy(usable_hbm.at[part], usable_ref.at[part], load_sem.at[piece, 1]),
        ])
        for copy in loads[-1]:
            copy.start()

    first = me == 0

    def rank_of(z):
        if isinstance(z, int):
            return n - 2 if z in (0, n - 1) else z - 1
        return jnp.where((z == 0) | (z == n - 1), n - 2, z - 1)

    rank = rank_of(me)

    def enter():
        @pl.when(rank > 0)
        def _():
            pl.semaphore_wait(barrier, 1)

        @pl.when(rank < n - 2)
        def _():
            pl.semaphore_signal(barrier, inc=1, device_id={"date": me + 1}, device_id_type=MESH)

        @pl.when(me == n - 2)
        def _():
            pl.semaphore_signal(barrier, inc=1, device_id={"date": 0}, device_id_type=MESH)

        for k in order:
            to = lax.rem(me + k, n)

            @pl.when(rank_of(to) < rank)
            def _():
                pl.semaphore_signal(known_sem.at[me], inc=1, device_id={"date": to}, device_id_type=MESH)

    def sample_copy(chunk, to, source):
        tiles = pl.ds(*CHUNKS[chunk])
        return pltpu.make_async_remote_copy(
            src_ref=send.at[to, tiles], dst_ref=recv.at[tiles, source], send_sem=send_sem.at[0], recv_sem=recv_sem.at[chunk, source],
            device_id={"date": to}, device_id_type=MESH,
        )

    def ready(half):
        for k in order:
            to = lax.rem(me + k, n)

            @pl.when((rank_of(to) < rank) & (to // (n // 2) == half))
            def _():
                sample_copy(0, to, me).start()

    pl.when(me > 0)(enter)
    pack(slc_ref, usable_ref, plane, split1, split2, send, loads, lambda: pl.when(first)(enter), ready, looks, dates)

    def send_lower():
        for k in order:
            to = lax.rem(me + k, n)

            @pl.when(rank_of(to) < rank)
            def _():
                sample_copy(1, to, me).start()

    late = n - LATE
    entry = [*range(1, n - 1), 0, n - 1]
    with jax.named_scope("start"):
        pl.when(rank < late)(send_lower)
        recv[:, me] = send[me]
        for place, z in enumerate(entry):

            @pl.when(rank < rank_of(z))
            def _():
                pl.semaphore_wait(known_sem.at[z], 1)
                for chunk in range(2 if place < late else 1):
                    sample_copy(chunk, z, me).start()

        @pl.when(me == n - 2)
        def _():
            pl.semaphore_signal(known_sem.at[0], inc=1, device_id={"date": n - 1}, device_id_type=MESH)
            pl.semaphore_signal(known_sem.at[n - 1], inc=1, device_id={"date": 0}, device_id_type=MESH)

        pl.when(rank >= late)(send_lower)
        for z in entry[late:]:

            @pl.when(rank < rank_of(z))
            def _():
                sample_copy(1, z, me).start()

        for one, other in ((0, n - 1), (n - 1, 0)):

            @pl.when(me == one)
            def _():
                pl.semaphore_wait(known_sem.at[other], 1)
                for chunk in range(2):
                    sample_copy(chunk, other, me).start()

    linked = []
    for chunk in range(2):
        with jax.named_scope("receive"):
            for k in order:
                source = lax.rem(me + n - k, n)
                sample_copy(chunk, source, source).wait_recv()
        members = [i for i in range(WINDOWS) if places(i)[0] == chunk]
        with jax.named_scope("gram"):
            sums = [gram(recv, coherence, i, looks) for i in members]
        with jax.named_scope("link"):
            linked.append(link(coherence, members, sums))
    vec_real, vec_imag = [
        jnp.concatenate([linked[chunk][c][half * PAIRS[chunk]:][:PAIRS[chunk]] for half in range(2) for chunk in range(2)], axis=0)
        for c in range(2)
    ]

    with jax.named_scope("note"):
        rows = jnp.concatenate([vec_real] + [vec_imag] * 4 + [vec_real] * 3, axis=0)
        turn[0:128] = rows.T
        lane = lane_iota((2 * n, 128))
        message = jnp.zeros((2 * n, 128), F32)
        for q in range(4):
            message = jnp.where((8 - lane // 16) % 4 == q, turn[pl.ds(q, 2 * n, stride=4), :], message)
        for d in range(n):
            note[d] = message[2 * d:2 * d + 2]

    def note_copy(k):
        to = lax.rem(me + k, n)
        return pltpu.make_async_remote_copy(
            src_ref=note.at[to], dst_ref=notes.at[me], send_sem=note_send.at[0], recv_sem=note_recv.at[k],
            device_id={"date": to}, device_id_type=MESH,
        )

    with jax.named_scope("notes"):
        for k in order:
            note_copy(k).start()
        notes[me] = note[me]
        pltpu.make_async_copy(send.at[0:n - 1], send.at[0:n - 1], send_sem.at[0]).wait()
        pltpu.make_async_copy(note.at[0:n - 1], note.at[0:n - 1], note_send.at[0]).wait()
        for k in order:
            source = lax.rem(me + n - k, n)
            pltpu.make_async_remote_copy(
                src_ref=note.at[source], dst_ref=notes.at[source], send_sem=note_send.at[0], recv_sem=note_recv.at[k],
                device_id={"date": source}, device_id_type=MESH,
            ).wait_recv()


def store(coherence, notes, coherence_out, linked_out, linked, sem):
    copies = [pltpu.make_async_copy(coherence.at[:, :, :, i], coherence_out.at[:, :, :, i], sem.at[i]) for i in range(WINDOWS)]
    for copy in copies:
        copy.start()
    lane = lane_iota((8, 128))
    for h in range(2):
        for half in range(2):
            tile = jnp.zeros((8, 128), F32)
            came = jnp.concatenate([notes[half * 8 + s, h:h + 1, :] for s in range(8)], axis=0)
            came = pltpu.roll(came, 0, 1, stride=16, stride_axis=0)
            for s in range(8):
                source = jnp.broadcast_to(came[s:s + 1], (8, 128))
                moved = pltpu.roll(source, 0, 1, stride=16, stride_axis=0)
                tile = jnp.where(lane // 16 == s, moved, tile)
            for c in range(2):
                linked[c, 4 * h:4 * h + 4, half * 128:half * 128 + 128] = tile[4 * c:4 * c + 4]
    copies.append(pltpu.make_async_copy(linked, linked_out, sem.at[WINDOWS]))
    copies[-1].start()
    for copy in copies:
        copy.wait()


def solution(mesh):
    n = mesh.shape["date"]

    def step(slc, usable):
        dates, windows = slc.shape[2], slc.shape[3]
        rows = 2 * slc.shape[1] * dates
        per_device = windows // n
        vmem, hbm = pl.BlockSpec(memory_space=pltpu.VMEM), pl.BlockSpec(memory_space=pl.ANY)
        coherence_shape, linked_shape = (2, 1, 1, per_device, n * dates, n * dates), (2, dates, windows)
        coherence, notes = pl.pallas_call(
            functools.partial(kernel, n),
            out_shape=(pltpu.VMEM(coherence_shape, BF16), pltpu.VMEM((n, 2, 128), F32)),
            in_specs=[hbm, hbm],
            out_specs=(vmem, vmem),
            scratch_shapes=[
                pltpu.VMEM(slc.shape, BF16),
                pltpu.VMEM(usable.shape, jnp.int32),
                pltpu.VMEM((windows // 128, rows + 8, 128), F32),
                pltpu.VMEM((windows * dates + 8, 128), F32),
                pltpu.VMEM((windows * dates // 2 + 8, 128), F32),
                pltpu.VMEM((n, TILES, dates, 128), BF16),
                pltpu.VMEM((TILES, n, dates, 128), BF16),
                pltpu.VMEM((136, 128), F32),
                pltpu.VMEM((n, 2, 128), F32),
                pltpu.SemaphoreType.DMA((LOADS, 2)),
                pltpu.SemaphoreType.DMA((1,)),
                pltpu.SemaphoreType.DMA((2, n)),
                pltpu.SemaphoreType.DMA((1,)),
                pltpu.SemaphoreType.DMA((n,)),
                pltpu.SemaphoreType.REGULAR((n,)),
            ],
            compiler_params=pltpu.CompilerParams(collective_id=0, has_side_effects=True),
        )(slc, usable)
        return pl.pallas_call(
            store,
            out_shape=(jax.ShapeDtypeStruct(coherence_shape, BF16), jax.ShapeDtypeStruct(linked_shape, F32)),
            in_specs=[vmem, vmem],
            out_specs=(hbm, hbm),
            scratch_shapes=[pltpu.VMEM(linked_shape, F32), pltpu.SemaphoreType.DMA((WINDOWS + 1,))],
        )(pltpu.with_memory_space_constraint(coherence, pltpu.VMEM), pltpu.with_memory_space_constraint(notes, pltpu.VMEM))

    return jax.shard_map(
        step,
        mesh=mesh,
        in_specs=(
            P(None, None, "date", ("slab", "tile", "sub")),
            P(None, "date", ("slab", "tile", "sub")),
        ),
        out_specs=(
            P(None, ("slab", "tile", "sub"), "date", None, None, None),
            P(None, "date", ("slab", "tile", "sub")),
        ),
        check_vma=False,
    )
```
